128 devices in a mesh: lat: 16 (over z, y_lo, core), lon: 8 (over y_hi, x).
Axes of the slice: x: 4, y: 4 (y_hi: 2, y_lo: 2; y = y_hi * 2 + y_lo), z: 4, core: 2. Of those that a mesh axis runs over, the one named last changes fastest.
Arguments:
- field: bfloat16 [256, 256, 256], P('lat', 'lon'), may hold values from -6 to 6
- weights: bfloat16 [16, 8, 3072, 3072], P('lat', 'lon'), may hold values from -0.09375 to 0.09375
- strip_ids: int32 [16, 8], P('lat'), may hold values from 0 to 63, as said below
- counts: int32 [16], P('lat'), may hold values from 2 to 8, as said below
Outputs:
- remapped: bfloat16 [131072, 256], P(('lat', 'lon'))
The draws below stay inside these ranges and needn't reach their ends.
Inputs may be any that keep to these rules, and one draw needn't show every extreme that they name: `strip_ids`: row b holds consecutive global strip numbers, the last one repeated where the run meets the end of its window, all among the strips of source bands b - 2 to b + 2, band c holding strips 4 * c to 4 * c + 3. Band b uses the first counts[b] slots of its row.
All inputs are finite; a program needn't handle non-finite values.
Results may differ from the reference program's by a relative error of at most 0.0059.
Values may be sent and summed in bfloat16 or wider, within the bound.
A program may use at most 64 MiB of HBM per device.

```python
import jax
import jax.numpy as jnp
from jax import lax

CHANNELS = 256
SRC_ROWS = 16
SRC_LON = 32
STRIP_ROWS = 4
STRIP_CELLS = 128
SLOTS = 8
REACH = 2
TGT_DEV = 1024
TGT_WIN = 3072
NUM_LAT = 256
NUM_LON = 256
NUM_TGT = 131072
N_LAT = 16
N_LON = 8


def strip_plan(key):
    per_device = SRC_ROWS // STRIP_ROWS
    strip_total = N_LAT * per_device
    band_index = jnp.arange(N_LAT, dtype=jnp.int32)
    lower = jnp.maximum(0, (band_index - REACH) * per_device)
    upper = jnp.minimum(strip_total, (band_index + REACH + 1) * per_device)
    drawn = jax.random.randint(jax.random.fold_in(key, 11), (N_LAT,), 2, SLOTS + 1)
    pattern = band_index % 4
    forced = (pattern == 0) | (pattern == 2)
    used = jnp.where(forced, SLOTS, drawn)
    room = upper - lower - used + 1
    offset = jax.random.randint(jax.random.fold_in(key, 12), (N_LAT,), 0, room)
    first_strip = lower + offset
    first_strip = jnp.where(pattern == 0, lower, jnp.where(pattern == 2, upper - SLOTS, first_strip))
    slot_range = jnp.arange(SLOTS, dtype=jnp.int32)
    chosen = jnp.minimum(first_strip[:, None] + slot_range[None, :], upper[:, None] - 1)
    return (chosen.astype(jnp.int32), used.astype(jnp.int32))


def draw_strip_ids(key, part):
    return strip_plan(key)[0]


def draw_counts(key, part):
    return strip_plan(key)[1]


def level_of(own_key, dims, shards, least, top_value):
    level, own = 1.0, jax.random.fold_in(own_key, 6)
    for position, parts in shards:
        draws = jnp.exp(jax.random.uniform(jax.random.fold_in(own, position), (parts,), jnp.float32, least / len(shards), top_value / len(shards)))
        level = level * jnp.repeat(draws, dims[position] // parts).reshape([-1 if axis == position else 1 for axis in range(len(dims))])
    return level


def normal_values(stream_key, shape, deviation, limit, shards=(), kind=jnp.bfloat16):
    values = jax.random.normal(stream_key, shape, jnp.float32) * deviation
    if len(shards) > 0:
        values = level_of(stream_key, shape, shards, -0.22, 0.18) * values
    return jnp.clip(values, min=-limit, max=limit).astype(kind)


def setup_inputs(seed: int = 0) -> dict:
    seeds = jax.random.split(jax.random.key(seed), 5)
    return {
        "field": normal_values(seeds[0], (NUM_LAT, NUM_LON, CHANNELS), 1.0, 6.0, ((0, 16), (1, 8))),
        "weights": normal_values(seeds[1], (N_LAT, N_LON, TGT_WIN, SLOTS * 3 * STRIP_CELLS), (3 * STRIP_CELLS * SLOTS * 3 // 2) ** -0.5, 0.09375, ((0, 16), (1, 8))),
        "strip_ids": draw_strip_ids(jax.random.fold_in(seeds[4], 71), 0),
        "counts": draw_counts(jax.random.fold_in(seeds[4], 71), 0),
    }


def reference(field, weights, strip_ids, counts):
    lon_wrapped = jnp.concatenate([field[:, -1:], field, field[:, :1]], axis=1)
    padded = jnp.concatenate([lon_wrapped[:1], lon_wrapped, lon_wrapped[-1:]], axis=0)
    values = padded.astype(jnp.float32)
    eastward = ((values[1:-1, 2:] - values[1:-1, :-2]) * 0.5).astype(jnp.bfloat16)
    northward = ((values[2:, 1:-1] - values[:-2, 1:-1]) * 0.5).astype(jnp.bfloat16)
    strip_total = NUM_LAT // STRIP_ROWS

    def sectorize(component):
        shaped = component.reshape(strip_total, STRIP_ROWS, N_LON, SRC_LON, CHANNELS)
        return shaped.transpose(0, 2, 1, 3, 4).reshape(strip_total, N_LON, STRIP_CELLS, CHANNELS)

    strips = jnp.stack([sectorize(field), sectorize(eastward), sectorize(northward)], axis=2)
    strips = strips.reshape(strip_total, N_LON, 3 * STRIP_CELLS, CHANNELS)
    slot_range = jnp.arange(SLOTS, dtype=jnp.int32)

    def band_rows(band_index):
        chosen = jnp.take(strips, strip_ids[band_index].astype(jnp.int32), axis=0)
        live_slots = slot_range < counts[band_index]
        chosen = jnp.where(live_slots[:, None, None, None], chosen, jnp.zeros_like(chosen))
        chosen = chosen.transpose(1, 0, 2, 3).reshape(N_LON, SLOTS * 3 * STRIP_CELLS, CHANNELS)
        weights_band = weights[band_index]

        def sector_partial(sector, collected):
            result = jnp.dot(weights_band[sector], chosen[sector], preferred_element_type=jnp.float32)
            return collected.at[sector].set(result)

        collected = lax.fori_loop(0, N_LON, sector_partial, jnp.zeros((N_LON, TGT_WIN, CHANNELS), jnp.float32))
        blocks = collected.reshape(N_LON, 3, TGT_DEV, CHANNELS)
        total = blocks[:, 1] + jnp.roll(blocks[:, 2], 1, axis=0) + jnp.roll(blocks[:, 0], -1, axis=0)
        return total.astype(jnp.bfloat16)

    mapped = lax.map(band_rows, jnp.arange(N_LAT, dtype=jnp.int32))
    return mapped.reshape(NUM_TGT, CHANNELS)
```

```python
import functools

import jax
import jax.numpy as jnp
from jax import lax
from jax.experimental import pallas as pl
from jax.experimental.pallas import tpu as pltpu
from jax.sharding import PartitionSpec as P

MESH = pl.DeviceIdType.MESH
F32 = jnp.float32
BF16 = jnp.bfloat16

ROWS = 16
LON = 32
CHAN = 256
STRIP_ROWS = 4
SLOTS = 8
CELLS = STRIP_ROWS * LON
DEPTH = 3 * CELLS
TGT = 1024
PARTS = 1
WIDTH = CHAN // PARTS
STEP = 256
STEPS = TGT // STEP
W_COPIES = 12
PIECES = 5


def kernel(
    ids_ref, counts_ref, field_ref, w_ref, out_ref,
    nb, rims, edge_out, edge_in, x_ref, w_vmem, centre, to_east, to_west, from_west, from_east,
    field_sem, w_sem,
    p_send, p_recv, z_send, z_recv, d_send, d_recv, f_send, f_recv, e_send, e_recv, r_send, r_recv,
    b_send, b_recv,
):
    lat = lax.axis_index("lat")
    lon = lax.axis_index("lon")
    core = lat % 2
    y_lo = (lat // 2) % 2
    sibling = lat + 1 - 2 * core
    partner = lat + 2 - 4 * y_lo
    relay_to = (lat + 4 - 8 * y_lo + 16) % 16
    relay_from = (lat - 4 + 8 * y_lo + 16) % 16
    above3 = (lat + 13) % 16
    below3 = (lat + 3) % 16
    east = (lon + 1) % 8
    west = (lon + 7) % 8

    def device(a, o):
        return (a, o)

    own = 1 + 2 * ROWS
    field_copies = []
    for h in range(PARTS):
        field_copies.append(
            pltpu.make_async_copy(
                field_ref.at[:, :, pl.ds(h * WIDTH, WIDTH)], nb.at[h, pl.ds(own, ROWS)], field_sem.at[h]
            )
        )
        field_copies[-1].start()

    barrier = pltpu.get_barrier_semaphore()
    peers = (
        (above3, lon), (below3, lon), (lat, east), (lat, west),
        (relay_to, lon), (relay_from, lon), (partner, lon), (sibling, lon),
    )
    for peer in peers:
        pl.semaphore_signal(barrier, inc=1, device_id=peer, device_id_type=MESH)

    w_rows = 3 * TGT // W_COPIES
    w_copies = []
    for i in range(W_COPIES):
        rows = pl.ds(i * w_rows, w_rows)
        w_copies.append(pltpu.make_async_copy(w_ref.at[0, 0, rows], w_vmem.at[rows], w_sem.at[i]))
        w_copies[-1].start()

    for copy in field_copies:
        copy.wait()
    row8 = lax.broadcasted_iota(jnp.int32, (8, WIDTH), 0)
    for h in range(PARTS):
        for q in range(4):
            first = jnp.zeros((8, WIDTH), F32)
            last = jnp.zeros((8, WIDTH), F32)
            for i in range(4):
                head = nb[h, own + 4 * q + i, 0:16].astype(F32)
                tail = nb[h, own + 4 * q + i, LON - 16 : LON].astype(F32)
                first = jnp.where(row8 == 4 + i, jnp.broadcast_to(head[0:1], (8, WIDTH)), first)
                last = jnp.where(row8 == i, jnp.broadcast_to(tail[15:16], (8, WIDTH)), last)
            edge_out[h, 0, q] = first.astype(BF16)
            edge_out[h, 1, q] = last.astype(BF16)

    pl.semaphore_wait(barrier, len(peers))

    pending = []

    def send(src, dst, send_sem, recv_sem, peer):
        copy = pltpu.make_async_remote_copy(
            src_ref=src, dst_ref=dst, send_sem=send_sem, recv_sem=recv_sem,
            device_id=peer, device_id_type=MESH,
        )
        copy.start()
        return copy

    def piece(h, slot, n):
        if n == PIECES - 1:
            return nb.at[h, pl.ds(1 + ROWS * slot + 12, 4)]
        if n == PIECES - 2:
            return rims.at[h, pl.ds(4 * slot, 4)]
        return nb.at[h, pl.ds(1 + ROWS * slot + 4 * n, 4)]

    def piece_copy(src, dst, send_sem, recv_sem, peer):
        return pltpu.make_async_remote_copy(
            src_ref=src, dst_ref=dst, send_sem=send_sem, recv_sem=recv_sem,
            device_id=peer, device_id_type=MESH,
        )

    p_slot = 4 * (1 - y_lo)
    q_slot = 4 * y_lo
    fwd_src = 4 * (1 - core)
    fwd_dst = 3 - 2 * core
    own_dst = 1 + 2 * core

    def p_copy(h, n):
        return piece_copy(piece(h, 2, n), piece(h, q_slot, n), p_send.at[h, n], p_recv.at[h, n], (partner, lon))

    def z_copy(h, n):
        return piece_copy(piece(h, p_slot, n), piece(h, q_slot, n), z_send.at[h, n], z_recv.at[h, n], (relay_to, lon))

    def d_copy(h, n):
        return piece_copy(piece(h, 2, n), piece(h, own_dst, n), d_send.at[h, n], d_recv.at[h, n], (sibling, lon))

    def f_copy(h, n):
        return piece_copy(piece(h, fwd_src, n), piece(h, fwd_dst, n), f_send.at[h, n], f_recv.at[h, n], (sibling, lon))

    def e_copies(h):
        return (
            piece_copy(edge_out.at[h, 0], edge_in.at[h, 0], e_send.at[h, 0], e_recv.at[h, 0], (lat, west)),
            piece_copy(edge_out.at[h, 1], edge_in.at[h, 1], e_send.at[h, 1], e_recv.at[h, 1], (lat, east)),
        )

    def r_copies(h):
        return (
            piece_copy(nb.at[h, pl.ds(own, 1)], nb.at[h, pl.ds(1 + 5 * ROWS, 1)], r_send.at[h, 0], r_recv.at[h, 0], (above3, lon)),
            piece_copy(nb.at[h, pl.ds(own + ROWS - 1, 1)], nb.at[h, pl.ds(0, 1)], r_send.at[h, 1], r_recv.at[h, 1], (below3, lon)),
        )

    for h in range(PARTS):
        for copy in e_copies(h):
            copy.start()
        for n in range(3):
            p_copy(h, n).start()
            d_copy(h, n).start()
        for copy in r_copies(h):
            copy.start()
    for h in range(PARTS):
        for copy in e_copies(h):
            copy.wait_recv()
        rims[h, 8:12] = edge_in[h, 0] + edge_in[h, 1]
        for n in (3, 4):
            p_copy(h, n).start()
            d_copy(h, n).start()

    def on_p(h, n):
        p_copy(h, n).wait_recv()
        z_copy(h, n).start()

        @pl.when(core == y_lo)
        def _():
            f_copy(h, n).start()

    def on_q(h, n):
        z_copy(h, n).wait_recv()

        @pl.when(core != y_lo)
        def _():
            f_copy(h, n).start()

    for h in range(PARTS):
        for n in range(PIECES):
            on_p(h, n)
            if n > 0:
                on_q(h, n - 1)
        on_q(h, PIECES - 1)

    column = lax.broadcasted_iota(jnp.int32, (LON, WIDTH), 0)

    def stencil(h):
        def slot(k, carry):
            strip = jnp.clip(ids_ref[0, k] - (lat - 2) * 4, 0, 19)
            live = k < counts_ref[0]
            base = strip * 4
            rim = rims[h, strip].astype(F32)
            rows = [nb[h, base + i].astype(F32) for i in range(6)]
            top = (lat - 2) * ROWS + base
            rows[0] = jnp.where(top == 0, rows[1], rows[0])
            rows[5] = jnp.where(top == 256 - STRIP_ROWS, rows[4], rows[5])
            at = k * DEPTH
            for i in range(4):
                centre_row = rows[i + 1]
                before = jnp.where(column == 0, jnp.broadcast_to(rim[i : i + 1], (LON, WIDTH)), pltpu.roll(centre_row, 1, 0))
                after = jnp.where(
                    column == LON - 1, jnp.broadcast_to(rim[4 + i : 5 + i], (LON, WIDTH)), pltpu.roll(centre_row, LON - 1, 0)
                )
                values = (centre_row, (after - before) * 0.5, (rows[i + 2] - rows[i]) * 0.5)
                for part, value in enumerate(values):
                    kept = jnp.where(live, value, jnp.zeros_like(value)).astype(BF16)
                    x_ref[h, pl.ds(pl.multiple_of(at + part * CELLS + i * LON, LON), LON)] = kept
            return carry

        lax.fori_loop(0, SLOTS, slot, 0)

    def b_copy(h, side, i, rows):
        src, dst, peer = (
            (to_east, from_west, (lat, east)) if side == 0 else (to_west, from_east, (lat, west))
        )
        return piece_copy(src.at[h, rows], dst.at[h, rows], b_send.at[h, side, i], b_recv.at[h, side, i], peer)

    for h in range(PARTS):
        if h == 0:
            for copy in w_copies:
                copy.wait()
        for n in range(PIECES):
            d_copy(h, n).wait_recv()
            f_copy(h, n).wait_recv()
        for copy in r_copies(h):
            copy.wait_recv()
        stencil(h)

        def outward(i, carry):
            at = pl.multiple_of(i * STEP, STEP)
            rows = pl.ds(at, STEP)
            for side, base, dst in ((0, 2 * TGT, to_east), (1, 0, to_west)):
                part = jnp.dot(w_vmem[pl.ds(base + at, STEP)], x_ref[h], preferred_element_type=F32)
                dst[h, rows] = part.astype(BF16)
                b_copy(h, side, i, rows).start()
            return carry

        lax.fori_loop(0, STEPS, outward, 0)

        def inward(i, carry):
            at = pl.multiple_of(i * STEP, STEP)
            rows = pl.ds(at, STEP)
            centre[h, rows] = jnp.dot(w_vmem[pl.ds(TGT + at, STEP)], x_ref[h], preferred_element_type=F32)
            return carry

        lax.fori_loop(0, STEPS, inward, 0)

    for h in range(PARTS):

        def finish(i, carry):
            at = pl.multiple_of(i * STEP, STEP)
            rows = pl.ds(at, STEP)
            for side in range(2):
                b_copy(h, side, i, rows).wait_recv()
            total = centre[h, rows] + from_west[h, rows].astype(F32) + from_east[h, rows].astype(F32)
            out_ref[rows, h * WIDTH : (h + 1) * WIDTH] = total.astype(BF16)
            return carry

        lax.fori_loop(0, STEPS, finish, 0)

    for h in range(PARTS):
        for n in range(PIECES):
            p_copy(h, n).wait_send()
            z_copy(h, n).wait_send()
            d_copy(h, n).wait_send()
            f_copy(h, n).wait_send()
        for copy in e_copies(h) + r_copies(h):
            copy.wait_send()

        def sent(i, carry):
            rows = pl.ds(pl.multiple_of(i * STEP, STEP), STEP)
            for side in range(2):
                b_copy(h, side, i, rows).wait_send()
            return carry

        lax.fori_loop(0, STEPS, sent, 0)


def body(field, weights, strip_ids, counts):
    dma = pltpu.SemaphoreType.DMA
    return pl.pallas_call(
        kernel,
        out_shape=jax.ShapeDtypeStruct((TGT, CHAN), BF16),
        in_specs=[
            pl.BlockSpec(memory_space=pltpu.SMEM),
            pl.BlockSpec(memory_space=pltpu.SMEM),
            pl.BlockSpec(memory_space=pltpu.HBM),
            pl.BlockSpec(memory_space=pltpu.HBM),
        ],
        out_specs=pl.BlockSpec(memory_space=pltpu.VMEM),
        scratch_shapes=[
            pltpu.VMEM((PARTS, 5 * ROWS + 2, LON, WIDTH), BF16),
            pltpu.VMEM((PARTS, 20, 8, WIDTH), BF16),
            pltpu.VMEM((PARTS, 2, 4, 8, WIDTH), BF16),
            pltpu.VMEM((PARTS, 2, 4, 8, WIDTH), BF16),
            pltpu.VMEM((PARTS, SLOTS * DEPTH, WIDTH), BF16),
            pltpu.VMEM((3 * TGT, SLOTS * DEPTH), BF16),
            pltpu.VMEM((PARTS, TGT, WIDTH), F32),
            pltpu.VMEM((PARTS, TGT, WIDTH), BF16),
            pltpu.VMEM((PARTS, TGT, WIDTH), BF16),
            pltpu.VMEM((PARTS, TGT, WIDTH), BF16),
            pltpu.VMEM((PARTS, TGT, WIDTH), BF16),
            dma((PARTS,)),
            dma((W_COPIES,)),
            dma((PARTS, PIECES)), dma((PARTS, PIECES)),
            dma((PARTS, PIECES)), dma((PARTS, PIECES)),
            dma((PARTS, PIECES)), dma((PARTS, PIECES)),
            dma((PARTS, PIECES)), dma((PARTS, PIECES)),
            dma((PARTS, 2)), dma((PARTS, 2)),
            dma((PARTS, 2)), dma((PARTS, 2)),
            dma((PARTS, 2, STEPS)), dma((PARTS, 2, STEPS)),
        ],
        compiler_params=pltpu.CompilerParams(
            collective_id=0, has_side_effects=True, vmem_limit_bytes=48 * 1024 * 1024
        ),
    )(strip_ids, counts, field, weights)


def solution(mesh):
    placed = (P("lat", "lon", None), P("lat", "lon", None, None), P("lat", None), P("lat"))
    return jax.shard_map(
        body, mesh=mesh, in_specs=placed, out_specs=P(("lat", "lon"), None), check_vma=False
    )
```

```python
import jax
import jax.numpy as jnp
from jax import lax
from jax.experimental import pallas as pl
from jax.experimental.pallas import tpu as pltpu
from jax.sharding import PartitionSpec as P

MESH = pl.DeviceIdType.MESH
F32 = jnp.float32
BF16 = jnp.bfloat16

N_LAT = 16
N_LON = 8
ROWS = 16
LON = 32
CHAN = 256
STRIP_ROWS = 4
SLOTS = 8
CELLS = STRIP_ROWS * LON
DEPTH = 3 * CELLS
TGT = 1024
PARTS = 2
WIDTH = CHAN // PARTS
STEP = 256
STEPS = TGT // STEP
W_COPIES = 12
PIECES = 4
OWN = 1 + 2 * ROWS
NEAR = (-2, -1, 1, 2)


def kernel(
    ids_hbm, counts_hbm, field_ref, w_ref, out_ref,
    ids_ref, counts_ref, nb_first, nb_second, rims, edge_out, edge_in, x_ref, w_vmem, centre,
    to_east, to_west, from_west, from_east,
    field_sem, w_sem, ids_sem,
    p_send, p_recv, z_send, z_recv, d_send, d_recv, f_send, f_recv,
    e_send, e_recv, m_send, m_recv, r_send, r_recv, b_send, b_recv,
):
    nb = (nb_first, nb_second)
    lat = lax.axis_index("lat")
    lon = lax.axis_index("lon")
    core = lat % 2
    y_lo = (lat // 2) % 2
    sibling = lat + 1 - 2 * core
    partner = lat + 2 - 4 * y_lo
    relay_to = lat + 4 - 8 * y_lo
    relay_from = lat - 4 + 8 * y_lo
    east = (lon + 1) % N_LON
    west = (lon + N_LON - 1) % N_LON

    def inside(a):
        return (a >= 0) & (a < N_LAT)

    has_relay_to = inside(relay_to)
    has_relay_from = inside(relay_from)

    field_copies = [
        pltpu.make_async_copy(
            field_ref.at[:, :, pl.ds(h * WIDTH, WIDTH)], nb[h].at[pl.ds(OWN, ROWS)], field_sem.at[h]
        )
        for h in range(PARTS)
    ]
    for copy in field_copies:
        copy.start()
    id_copies = (
        pltpu.make_async_copy(ids_hbm, ids_ref, ids_sem.at[0]),
        pltpu.make_async_copy(counts_hbm, counts_ref, ids_sem.at[1]),
    )
    for copy in id_copies:
        copy.start()

    barrier = pltpu.get_barrier_semaphore()
    for peer in (east, west):
        pl.semaphore_signal(barrier, inc=1, device_id=(lat, peer), device_id_type=MESH)
    arrivals = 2
    for d in (-4, 4, -3, 3, -2, 2, -1, 1):

        @pl.when(inside(lat + d))
        def _(d=d):
            pl.semaphore_signal(barrier, inc=1, device_id=(lat + d, lon), device_id_type=MESH)

        arrivals = arrivals + jnp.where(inside(lat + d), 1, 0)

    w_rows = 3 * TGT // W_COPIES
    w_copies = []
    for i in range(W_COPIES):
        rows = pl.ds(i * w_rows, w_rows)
        w_copies.append(pltpu.make_async_copy(w_ref.at[0, 0, rows], w_vmem.at[rows], w_sem.at[i]))
        w_copies[-1].start()

    for copy in field_copies:
        copy.wait()
    row8 = lax.broadcasted_iota(jnp.int32, (8, WIDTH), 0)
    for h in range(PARTS):
        for q in range(4):
            first = jnp.zeros((8, WIDTH), F32)
            last = jnp.zeros((8, WIDTH), F32)
            for i in range(4):
                head = nb[h][OWN + 4 * q + i, 0:16].astype(F32)
                tail = nb[h][OWN + 4 * q + i, LON - 16 : LON].astype(F32)
                first = jnp.where(row8 == 4 + i, jnp.broadcast_to(head[0:1], (8, WIDTH)), first)
                last = jnp.where(row8 == i, jnp.broadcast_to(tail[15:16], (8, WIDTH)), last)
            edge_out[0, q, h] = first.astype(BF16)
            edge_out[1, q, h] = last.astype(BF16)

    with jax.named_scope("barrier"):
        pl.semaphore_wait(barrier, arrivals)

    def remote(src, dst, send_sem, recv_sem, peer):
        return pltpu.make_async_remote_copy(
            src_ref=src, dst_ref=dst, send_sem=send_sem, recv_sem=recv_sem,
            device_id=peer, device_id_type=MESH,
        )

    def piece(h, slot, n):
        return nb[h].at[pl.ds(1 + ROWS * slot + 4 * n, 4)]

    p_slot = 4 * (1 - y_lo)
    q_slot = 4 * y_lo
    fwd_src = 4 * (1 - core)
    fwd_dst = 3 - 2 * core
    own_dst = 1 + 2 * core

    def p_copy(h, n):
        return remote(piece(h, 2, n), piece(h, q_slot, n), p_send.at[h, n], p_recv.at[h, n], (partner, lon))

    def z_copy(h, n):
        return remote(piece(h, p_slot, n), piece(h, q_slot, n), z_send.at[h, n], z_recv.at[h, n], (relay_to, lon))

    def d_copy(h, n):
        return remote(piece(h, 2, n), piece(h, own_dst, n), d_send.at[h, n], d_recv.at[h, n], (sibling, lon))

    def f_copy(h, n):
        return remote(piece(h, fwd_src, n), piece(h, fwd_dst, n), f_send.at[h, n], f_recv.at[h, n], (sibling, lon))

    e_copies = (
        remote(edge_out.at[0], edge_in.at[0], e_send.at[0], e_recv.at[0], (lat, west)),
        remote(edge_out.at[1], edge_in.at[1], e_send.at[1], e_recv.at[1], (lat, east)),
    )

    def m_copy(d):
        slot = 2 - d
        return remote(
            rims.at[pl.ds(8, 4)], rims.at[pl.ds(4 * slot, 4)], m_send.at[slot], m_recv.at[slot], (lat + d, lon)
        )

    def up_copy(h):
        src, dst = nb[h].at[pl.ds(OWN, 1)], nb[h].at[pl.ds(1 + 5 * ROWS, 1)]
        return remote(src, dst, r_send.at[h, 0], r_recv.at[h, 0], (lat - 3, lon))

    def down_copy(h):
        src, dst = nb[h].at[pl.ds(OWN + ROWS - 1, 1)], nb[h].at[pl.ds(0, 1)]
        return remote(src, dst, r_send.at[h, 1], r_recv.at[h, 1], (lat + 3, lon))

    for copy in e_copies:
        copy.start()
    def send_own(h):
        for n in range(PIECES):
            p_copy(h, n).start()
            d_copy(h, n).start()
        pl.when(inside(lat - 3))(lambda: up_copy(h).start())
        pl.when(inside(lat + 3))(lambda: down_copy(h).start())

    send_own(0)

    has_fwd_out = ((core == 0) & (lat < 14)) | ((core == 1) & (lat >= 2))
    has_fwd_in = ((core == 1) & (lat < 14)) | ((core == 0) & (lat >= 2))

    def on_p(h, n):
        p_copy(h, n).wait_recv()
        pl.when(has_relay_to)(lambda: z_copy(h, n).start())
        pl.when(core == y_lo)(lambda: f_copy(h, n).start())

    def on_q(h):
        @pl.when(has_relay_from)
        def _():
            for n in range(PIECES):
                z_copy(h, n).wait_recv()
                pl.when(core != y_lo)(lambda n=n: f_copy(h, n).start())

    def tiles_in(h):
        for n in range(PIECES):
            d_copy(h, n).wait_recv()
        pl.when(inside(lat + 3))(lambda: up_copy(h).wait_recv())
        pl.when(inside(lat - 3))(lambda: down_copy(h).wait_recv())

        @pl.when(has_fwd_in)
        def _():
            for n in range(PIECES):
                f_copy(h, n).wait_recv()

    column = lax.broadcasted_iota(jnp.int32, (LON, WIDTH), 0)

    def stencil(h):
        def slot(k, carry):
            strip = jnp.clip(ids_ref[0, k] - (lat - 2) * 4, 0, 19)
            live = k < counts_ref[0]
            base = strip * 4
            rim = rims[strip, h].astype(F32)
            rows = [nb[h][base + i].astype(F32) for i in range(6)]
            top = (lat - 2) * ROWS + base
            rows[0] = jnp.where(top == 0, rows[1], rows[0])
            rows[5] = jnp.where(top == N_LAT * ROWS - STRIP_ROWS, rows[4], rows[5])
            at = k * DEPTH
            for i in range(4):
                mid = rows[i + 1]
                before = jnp.where(column == 0, jnp.broadcast_to(rim[i : i + 1], (LON, WIDTH)), pltpu.roll(mid, 1, 0))
                after = jnp.where(
                    column == LON - 1, jnp.broadcast_to(rim[4 + i : 5 + i], (LON, WIDTH)), pltpu.roll(mid, LON - 1, 0)
                )
                values = (mid, (after - before) * 0.5, (rows[i + 2] - rows[i]) * 0.5)
                for part, value in enumerate(values):
                    kept = jnp.where(live, value, jnp.zeros_like(value)).astype(BF16)
                    cells = pl.ds(pl.multiple_of(at + part * CELLS + i * LON, LON), LON)
                    x_ref[cells, h * WIDTH : (h + 1) * WIDTH] = kept
            return carry

        with jax.named_scope("stencil"):
            lax.fori_loop(0, SLOTS, slot, 0)

    def b_copy(h, side, i):
        rows = pl.ds(i * STEP, STEP)
        if side == 0:
            return remote(to_east.at[h, rows], from_west.at[h, rows], b_send.at[h, 0, i], b_recv.at[h, 0, i], (lat, east))
        return remote(to_west.at[h, rows], from_east.at[h, rows], b_send.at[h, 1, i], b_recv.at[h, 1, i], (lat, west))

    def outward(h, i):
        with jax.named_scope("outward"):
            at = i * STEP
            x = x_ref[:, h * WIDTH : (h + 1) * WIDTH]
            for_east = jnp.dot(w_vmem[pl.ds(2 * TGT + at, STEP)], x, preferred_element_type=F32)
            for_west = jnp.dot(w_vmem[pl.ds(at, STEP)], x, preferred_element_type=F32)
            to_east[h, pl.ds(at, STEP)] = for_east.astype(BF16)
            to_west[h, pl.ds(at, STEP)] = for_west.astype(BF16)
            b_copy(h, 0, i).start()
            b_copy(h, 1, i).start()

    with jax.named_scope("relay0"):
        on_p(0, 0)
        on_p(0, 1)
        for copy in e_copies:
            copy.wait_recv()
        rims[8:12] = edge_in[0] + edge_in[1]
        for d in NEAR:
            pl.when(inside(lat + d))(lambda d=d: m_copy(d).start())
        send_own(1)
        for n in range(2, PIECES):
            on_p(0, n)
    with jax.named_scope("q0"):
        on_q(0)
    with jax.named_scope("weights"):
        for copy in (*w_copies, *id_copies):
            copy.wait()
    with jax.named_scope("rims"):
        for d in NEAR:
            pl.when(inside(lat - d))(lambda d=d: m_copy(d).wait_recv())
    with jax.named_scope("tiles0"):
        tiles_in(0)
    stencil(0)
    outward(0, 0)
    for h in range(1, PARTS):
        with jax.named_scope("p1"):
            for n in range(PIECES):
                on_p(h, n)
        outward(h - 1, 1)
        outward(h - 1, 2)
        with jax.named_scope("q1"):
            on_q(h)
        outward(h - 1, 3)
        with jax.named_scope("tiles1"):
            tiles_in(h)
        stencil(h)
        outward(h, 0)
    for i in range(1, STEPS):
        outward(PARTS - 1, i)
    with jax.named_scope("inward"):
        half = TGT // 2
        x = x_ref[...]
        upper = jnp.dot(w_vmem[pl.ds(TGT, half)], x, preferred_element_type=F32)
        lower = jnp.dot(w_vmem[pl.ds(TGT + half, half)], x, preferred_element_type=F32)
        centre[:half] = upper
        centre[half:] = lower

    for h in range(PARTS):
        columns = pl.ds(h * WIDTH, WIDTH)
        for i in range(STEPS):
            with jax.named_scope("finish"):
                rows = pl.ds(i * STEP, STEP)
                for side in range(2):
                    b_copy(h, side, i).wait_recv()
                total = centre[rows, columns] + from_west[h, rows].astype(F32) + from_east[h, rows].astype(F32)
                out_ref[rows, columns] = total.astype(BF16)

    with jax.named_scope("tail"):
        for h in range(PARTS):
            for n in range(PIECES):
                p_copy(h, n).wait_send()
                d_copy(h, n).wait_send()
                pl.when(has_relay_to)(lambda h=h, n=n: z_copy(h, n).wait_send())
                pl.when(has_fwd_out)(lambda h=h, n=n: f_copy(h, n).wait_send())
            for i in range(STEPS):
                for side in range(2):
                    b_copy(h, side, i).wait_send()
        for copy in e_copies:
            copy.wait_send()
        for d in NEAR:
            pl.when(inside(lat + d))(lambda d=d: m_copy(d).wait_send())
        for h in range(PARTS):
            pl.when(inside(lat - 3))(lambda h=h: up_copy(h).wait_send())
            pl.when(inside(lat + 3))(lambda h=h: down_copy(h).wait_send())


def body(field, weights, strip_ids, counts):
    dma = pltpu.SemaphoreType.DMA
    field, weights, strip_ids = (
        pltpu.with_memory_space_constraint(a, pltpu.HBM) for a in (field, weights, strip_ids)
    )
    return pl.pallas_call(
        kernel,
        out_shape=jax.ShapeDtypeStruct((TGT, CHAN), BF16),
        in_specs=[pl.BlockSpec(memory_space=pl.ANY)] * 4,
        out_specs=pl.BlockSpec(memory_space=pltpu.VMEM),
        scratch_shapes=[
            pltpu.SMEM((1, SLOTS), jnp.int32),
            pltpu.SMEM((1,), jnp.int32),
            pltpu.VMEM((5 * ROWS + 2, LON, WIDTH), BF16),
            pltpu.VMEM((5 * ROWS + 2, LON, WIDTH), BF16),
            pltpu.VMEM((20, PARTS, 8, WIDTH), BF16),
            pltpu.VMEM((2, 4, PARTS, 8, WIDTH), BF16),
            pltpu.VMEM((2, 4, PARTS, 8, WIDTH), BF16),
            pltpu.VMEM((SLOTS * DEPTH, CHAN), BF16),
            pltpu.VMEM((3 * TGT, SLOTS * DEPTH), BF16),
            pltpu.VMEM((TGT, CHAN), F32),
            pltpu.VMEM((PARTS, TGT, WIDTH), BF16),
            pltpu.VMEM((PARTS, TGT, WIDTH), BF16),
            pltpu.VMEM((PARTS, TGT, WIDTH), BF16),
            pltpu.VMEM((PARTS, TGT, WIDTH), BF16),
            dma((PARTS,)), dma((W_COPIES,)), dma((2,)),
            dma((PARTS, PIECES)), dma((PARTS, PIECES)),
            dma((PARTS, PIECES)), dma((PARTS, PIECES)),
            dma((PARTS, PIECES)), dma((PARTS, PIECES)),
            dma((PARTS, PIECES)), dma((PARTS, PIECES)),
            dma((2,)), dma((2,)),
            dma((5,)), dma((5,)),
            dma((PARTS, 2)), dma((PARTS, 2)),
            dma((PARTS, 2, STEPS)), dma((PARTS, 2, STEPS)),
        ],
        compiler_params=pltpu.CompilerParams(
            collective_id=0, has_side_effects=True, vmem_limit_bytes=48 * 1024 * 1024
        ),
    )(strip_ids, counts, field, weights)


def solution(mesh):
    placed = (P("lat", "lon", None), P("lat", "lon", None, None), P("lat", None), P("lat"))
    return jax.shard_map(
        body, mesh=mesh, in_specs=placed, out_specs=P(("lat", "lon"), None), check_vma=False
    )
```

```python
import jax
import jax.numpy as jnp
from jax import lax
from jax.experimental import pallas as pl
from jax.experimental.pallas import tpu as pltpu
from jax.sharding import PartitionSpec as P

MESH = pl.DeviceIdType.MESH
F32 = jnp.float32
BF16 = jnp.bfloat16

N_LAT = 16
N_LON = 8
ROWS = 16
LON = 32
CHAN = 256
STRIP_ROWS = 4
SLOTS = 8
CELLS = STRIP_ROWS * LON
DEPTH = 3 * CELLS
TGT = 1024
PARTS = 2
WIDTH = CHAN // PARTS
STEP = 256
STEPS = TGT // STEP
W_COPIES = 12
PIECES = 4
OWN = 1 + 2 * ROWS
NEAR = (-2, -1, 1, 2)


def kernel(
    ids_hbm, counts_hbm, field_ref, w_ref, out_ref,
    ids_ref, counts_ref, nb_first, nb_second, rims, edge_out, edge_in, x_ref, w_vmem, centre,
    to_east, to_west, from_west, from_east,
    field_sem, w_sem, ids_sem, ready_sem,
    p_send, p_recv, z_send, z_recv, d_send, d_recv, f_send, f_recv,
    e_send, e_recv, m_send, m_recv, r_send, r_recv, b_send, b_recv,
):
    nb = (nb_first, nb_second)
    lat = lax.axis_index("lat")
    lon = lax.axis_index("lon")
    core = lat % 2
    y_lo = (lat // 2) % 2
    sibling = lat + 1 - 2 * core
    partner = lat + 2 - 4 * y_lo
    relay_to = lat + 4 - 8 * y_lo
    relay_from = lat - 4 + 8 * y_lo
    east = (lon + 1) % N_LON
    west = (lon + N_LON - 1) % N_LON

    def inside(a):
        return (a >= 0) & (a < N_LAT)

    has_relay_to = inside(relay_to)
    has_relay_from = inside(relay_from)

    field_copies = [
        pltpu.make_async_copy(
            field_ref.at[:, :, pl.ds(h * WIDTH, WIDTH)], nb[h].at[pl.ds(OWN, ROWS)], field_sem.at[h]
        )
        for h in range(PARTS)
    ]
    for copy in field_copies:
        copy.start()
    id_copies = (
        pltpu.make_async_copy(ids_hbm, ids_ref, ids_sem.at[0]),
        pltpu.make_async_copy(counts_hbm, counts_ref, ids_sem.at[1]),
    )
    for copy in id_copies:
        copy.start()

    barrier = pltpu.get_barrier_semaphore()
    x_pos = lon % 4
    at_end = (x_pos == 0) | (x_pos == 3)
    across_x = jnp.where(x_pos == 0, lon + 3, lon - 3)
    across_y = (lon + 4) % N_LON
    for valid, peer in ((x_pos != 3, east), (x_pos != 0, west), (at_end, across_x), (at_end, across_y)):

        @pl.when(valid)
        def _(peer=peer):
            pl.semaphore_signal(barrier, inc=1, device_id=(lat, peer), device_id_type=MESH)

    arrivals = jnp.where(at_end, 3, 2)
    for d in (-4, 4, -3, 3, -2, 2, -1, 1):

        @pl.when(inside(lat + d))
        def _(d=d):
            pl.semaphore_signal(barrier, inc=1, device_id=(lat + d, lon), device_id_type=MESH)

        arrivals = arrivals + jnp.where(inside(lat + d), 1, 0)

    w_rows = 3 * TGT // W_COPIES
    w_copies = []
    for i in range(W_COPIES):
        rows = pl.ds(i * w_rows, w_rows)
        w_copies.append(pltpu.make_async_copy(w_ref.at[0, 0, rows], w_vmem.at[rows], w_sem.at[i]))
        w_copies[-1].start()

    for copy in field_copies:
        copy.wait()
    row8 = lax.broadcasted_iota(jnp.int32, (8, WIDTH), 0)
    for h in range(PARTS):
        for q in range(4):
            first = jnp.zeros((8, WIDTH), F32)
            last = jnp.zeros((8, WIDTH), F32)
            for i in range(4):
                head = nb[h][OWN + 4 * q + i, 0:16].astype(F32)
                tail = nb[h][OWN + 4 * q + i, LON - 16 : LON].astype(F32)
                first = jnp.where(row8 == 4 + i, jnp.broadcast_to(head[0:1], (8, WIDTH)), first)
                last = jnp.where(row8 == i, jnp.broadcast_to(tail[15:16], (8, WIDTH)), last)
            edge_out[0, q, h] = first.astype(BF16)
            edge_out[1, q, h] = last.astype(BF16)

    with jax.named_scope("barrier"):
        pl.semaphore_wait(barrier, arrivals)

    @pl.when(at_end)
    def _():
        pl.semaphore_signal(ready_sem, inc=1, device_id=(lat, across_y), device_id_type=MESH)

    def remote(src, dst, send_sem, recv_sem, peer):
        return pltpu.make_async_remote_copy(
            src_ref=src, dst_ref=dst, send_sem=send_sem, recv_sem=recv_sem,
            device_id=peer, device_id_type=MESH,
        )

    def piece(h, slot, n):
        return nb[h].at[pl.ds(1 + ROWS * slot + 4 * n, 4)]

    p_slot = 4 * (1 - y_lo)
    q_slot = 4 * y_lo
    fwd_src = 4 * (1 - core)
    fwd_dst = 3 - 2 * core
    own_dst = 1 + 2 * core

    def p_copy(h, n):
        return remote(piece(h, 2, n), piece(h, q_slot, n), p_send.at[h, n], p_recv.at[h, n], (partner, lon))

    def z_copy(h, n):
        return remote(piece(h, p_slot, n), piece(h, q_slot, n), z_send.at[h, n], z_recv.at[h, n], (relay_to, lon))

    def d_copy(h, n):
        return remote(piece(h, 2, n), piece(h, own_dst, n), d_send.at[h, n], d_recv.at[h, n], (sibling, lon))

    def f_copy(h, n):
        return remote(piece(h, fwd_src, n), piece(h, fwd_dst, n), f_send.at[h, n], f_recv.at[h, n], (sibling, lon))

    e_copies = (
        remote(edge_out.at[0], edge_in.at[0], e_send.at[0], e_recv.at[0], (lat, west)),
        remote(edge_out.at[1], edge_in.at[1], e_send.at[1], e_recv.at[1], (lat, east)),
    )

    def m_copy(d):
        slot = 2 - d
        return remote(
            rims.at[pl.ds(8, 4)], rims.at[pl.ds(4 * slot, 4)], m_send.at[slot], m_recv.at[slot], (lat + d, lon)
        )

    def up_copy(h):
        src, dst = nb[h].at[pl.ds(OWN, 1)], nb[h].at[pl.ds(1 + 5 * ROWS, 1)]
        return remote(src, dst, r_send.at[h, 0], r_recv.at[h, 0], (lat - 3, lon))

    def down_copy(h):
        src, dst = nb[h].at[pl.ds(OWN + ROWS - 1, 1)], nb[h].at[pl.ds(0, 1)]
        return remote(src, dst, r_send.at[h, 1], r_recv.at[h, 1], (lat + 3, lon))

    def send_own(h):
        for n in range(PIECES):
            p_copy(h, n).start()
            d_copy(h, n).start()
        pl.when(inside(lat - 3))(lambda: up_copy(h).start())
        pl.when(inside(lat + 3))(lambda: down_copy(h).start())

    send_own(0)
    send_own(1)
    with jax.named_scope("ready"):

        @pl.when(at_end)
        def _():
            pl.semaphore_wait(ready_sem, 1)

    for copy in e_copies:
        copy.start()

    has_fwd_out = ((core == 0) & (lat < 14)) | ((core == 1) & (lat >= 2))
    has_fwd_in = ((core == 1) & (lat < 14)) | ((core == 0) & (lat >= 2))

    def on_p(h, n):
        p_copy(h, n).wait_recv()
        pl.when(has_relay_to)(lambda: z_copy(h, n).start())
        pl.when(core == y_lo)(lambda: f_copy(h, n).start())

    def on_q(h, n):
        @pl.when(has_relay_from)
        def _():
            z_copy(h, n).wait_recv()
            pl.when(core != y_lo)(lambda: f_copy(h, n).start())

    def tiles_in(h):
        for n in range(PIECES):
            d_copy(h, n).wait_recv()
        pl.when(inside(lat + 3))(lambda: up_copy(h).wait_recv())
        pl.when(inside(lat - 3))(lambda: down_copy(h).wait_recv())

        @pl.when(has_fwd_in)
        def _():
            for n in range(PIECES):
                f_copy(h, n).wait_recv()

    column = lax.broadcasted_iota(jnp.int32, (LON, WIDTH), 0)

    def stencil(h):
        def slot(k, carry):
            strip = jnp.clip(ids_ref[0, k] - (lat - 2) * 4, 0, 19)
            live = k < counts_ref[0]
            base = strip * 4
            rim = rims[strip, h].astype(F32)
            rows = [nb[h][base + i].astype(F32) for i in range(6)]
            top = (lat - 2) * ROWS + base
            rows[0] = jnp.where(top == 0, rows[1], rows[0])
            rows[5] = jnp.where(top == N_LAT * ROWS - STRIP_ROWS, rows[4], rows[5])
            at = k * DEPTH
            for i in range(4):
                mid = rows[i + 1]
                before = jnp.where(column == 0, jnp.broadcast_to(rim[i : i + 1], (LON, WIDTH)), pltpu.roll(mid, 1, 0))
                after = jnp.where(
                    column == LON - 1, jnp.broadcast_to(rim[4 + i : 5 + i], (LON, WIDTH)), pltpu.roll(mid, LON - 1, 0)
                )
                values = (mid, (after - before) * 0.5, (rows[i + 2] - rows[i]) * 0.5)
                for part, value in enumerate(values):
                    kept = jnp.where(live, value, jnp.zeros_like(value)).astype(BF16)
                    cells = pl.ds(pl.multiple_of(at + part * CELLS + i * LON, LON), LON)
                    x_ref[cells, h * WIDTH : (h + 1) * WIDTH] = kept
            return carry

        with jax.named_scope("stencil"):
            lax.fori_loop(0, SLOTS, slot, 0)

    def b_copy(h, side, i):
        rows = pl.ds(i * STEP, STEP)
        if side == 0:
            return remote(to_east.at[h, rows], from_west.at[h, rows], b_send.at[h, 0, i], b_recv.at[h, 0, i], (lat, east))
        return remote(to_west.at[h, rows], from_east.at[h, rows], b_send.at[h, 1, i], b_recv.at[h, 1, i], (lat, west))

    def outward(h, i):
        with jax.named_scope("outward"):
            at = i * STEP
            x = x_ref[:, h * WIDTH : (h + 1) * WIDTH]
            for_east = jnp.dot(w_vmem[pl.ds(2 * TGT + at, STEP)], x, preferred_element_type=F32)
            for_west = jnp.dot(w_vmem[pl.ds(at, STEP)], x, preferred_element_type=F32)
            to_east[h, pl.ds(at, STEP)] = for_east.astype(BF16)
            to_west[h, pl.ds(at, STEP)] = for_west.astype(BF16)
            b_copy(h, 0, i).start()
            b_copy(h, 1, i).start()

    with jax.named_scope("relay0"):
        for n in range(PIECES):
            on_p(0, n)
    with jax.named_scope("edges"):
        for copy in e_copies:
            copy.wait_recv()
        rims[8:12] = edge_in[0] + edge_in[1]
        for d in NEAR:
            pl.when(inside(lat + d))(lambda d=d: m_copy(d).start())
    with jax.named_scope("q0"):
        for n in range(PIECES):
            on_q(0, n)
            if n + 1 < PIECES:
                on_p(1, n)
    with jax.named_scope("weights"):
        for copy in (*w_copies, *id_copies):
            copy.wait()
    with jax.named_scope("rims"):
        for d in NEAR:
            pl.when(inside(lat - d))(lambda d=d: m_copy(d).wait_recv())
    with jax.named_scope("tiles0"):
        tiles_in(0)
    stencil(0)
    outward(0, 0)
    with jax.named_scope("p1"):
        on_p(1, PIECES - 1)
    outward(0, 1)
    outward(0, 2)
    with jax.named_scope("q1"):
        for n in range(PIECES):
            on_q(1, n)
    outward(0, 3)
    with jax.named_scope("tiles1"):
        tiles_in(1)
    stencil(1)
    for i in range(STEPS):
        outward(1, i)
    with jax.named_scope("inward"):
        half = TGT // 2
        x = x_ref[...]
        upper = jnp.dot(w_vmem[pl.ds(TGT, half)], x, preferred_element_type=F32)
        lower = jnp.dot(w_vmem[pl.ds(TGT + half, half)], x, preferred_element_type=F32)
        centre[:half] = upper
        centre[half:] = lower

    for h in range(PARTS):
        columns = pl.ds(h * WIDTH, WIDTH)
        for i in range(STEPS):
            with jax.named_scope("finish"):
                rows = pl.ds(i * STEP, STEP)
                for side in range(2):
                    b_copy(h, side, i).wait_recv()
                total = centre[rows, columns] + from_west[h, rows].astype(F32) + from_east[h, rows].astype(F32)
                out_ref[rows, columns] = total.astype(BF16)

    with jax.named_scope("tail"):
        for h in range(PARTS):
            for n in range(PIECES):
                p_copy(h, n).wait_send()
                d_copy(h, n).wait_send()
                pl.when(has_relay_to)(lambda h=h, n=n: z_copy(h, n).wait_send())
                pl.when(has_fwd_out)(lambda h=h, n=n: f_copy(h, n).wait_send())
            for i in range(STEPS):
                for side in range(2):
                    b_copy(h, side, i).wait_send()
        for copy in e_copies:
            copy.wait_send()
        for d in NEAR:
            pl.when(inside(lat + d))(lambda d=d: m_copy(d).wait_send())
        for h in range(PARTS):
            pl.when(inside(lat - 3))(lambda h=h: up_copy(h).wait_send())
            pl.when(inside(lat + 3))(lambda h=h: down_copy(h).wait_send())


def body(field, weights, strip_ids, counts):
    dma = pltpu.SemaphoreType.DMA
    field, weights, strip_ids = (
        pltpu.with_memory_space_constraint(a, pltpu.HBM) for a in (field, weights, strip_ids)
    )
    return pl.pallas_call(
        kernel,
        out_shape=jax.ShapeDtypeStruct((TGT, CHAN), BF16),
        in_specs=[pl.BlockSpec(memory_space=pl.ANY)] * 4,
        out_specs=pl.BlockSpec(memory_space=pltpu.VMEM),
        scratch_shapes=[
            pltpu.SMEM((1, SLOTS), jnp.int32),
            pltpu.SMEM((1,), jnp.int32),
            pltpu.VMEM((5 * ROWS + 2, LON, WIDTH), BF16),
            pltpu.VMEM((5 * ROWS + 2, LON, WIDTH), BF16),
            pltpu.VMEM((20, PARTS, 8, WIDTH), BF16),
            pltpu.VMEM((2, 4, PARTS, 8, WIDTH), BF16),
            pltpu.VMEM((2, 4, PARTS, 8, WIDTH), BF16),
            pltpu.VMEM((SLOTS * DEPTH, CHAN), BF16),
            pltpu.VMEM((3 * TGT, SLOTS * DEPTH), BF16),
            pltpu.VMEM((TGT, CHAN), F32),
            pltpu.VMEM((PARTS, TGT, WIDTH), BF16),
            pltpu.VMEM((PARTS, TGT, WIDTH), BF16),
            pltpu.VMEM((PARTS, TGT, WIDTH), BF16),
            pltpu.VMEM((PARTS, TGT, WIDTH), BF16),
            dma((PARTS,)), dma((W_COPIES,)), dma((2,)), pltpu.SemaphoreType.REGULAR,
            dma((PARTS, PIECES)), dma((PARTS, PIECES)),
            dma((PARTS, PIECES)), dma((PARTS, PIECES)),
            dma((PARTS, PIECES)), dma((PARTS, PIECES)),
            dma((PARTS, PIECES)), dma((PARTS, PIECES)),
            dma((2,)), dma((2,)),
            dma((5,)), dma((5,)),
            dma((PARTS, 2)), dma((PARTS, 2)),
            dma((PARTS, 2, STEPS)), dma((PARTS, 2, STEPS)),
        ],
        compiler_params=pltpu.CompilerParams(
            collective_id=0, has_side_effects=True, vmem_limit_bytes=48 * 1024 * 1024
        ),
    )(strip_ids, counts, field, weights)


def solution(mesh):
    placed = (P("lat", "lon", None), P("lat", "lon", None, None), P("lat", None), P("lat"))
    return jax.shard_map(
        body, mesh=mesh, in_specs=placed, out_specs=P(("lat", "lon"), None), check_vma=False
    )
```
